32 devices in a mesh: gx: 4 (over x, core), gy: 4 (over z), gz: 2 (over y).
Axes of the slice: x: 2, y: 2, z: 4, core: 2. Of those that a mesh axis runs over, the one named last changes fastest.
Arguments:
- embeds: bfloat16 [256, 128, 2048], P(('gx', 'gy', 'gz')), may hold values from -6 to 6
- dest_device: int32 [256], P(('gx', 'gy', 'gz')), may hold values from 0 to 31, as said below
- shuffle_key: int32 [256], P(('gx', 'gy', 'gz')), may hold values from 0 to 255, each once
- lengths: int32 [8], replicated, may hold values from 1 to 4096
- gain: float32 [2048], replicated, may hold values from 0.1 to 1.9
Outputs:
- packed: bfloat16 [512, 128, 2048], P(('gx', 'gy', 'gz'))
The draws below stay inside these ranges and needn't reach their ends.
Inputs may be any that keep to these rules, and one draw needn't show every extreme that they name: `dest_device`: device numbers are ((gx * 4) + gy) * 2 + gz. A device receives at most 16 tiles, and in every draw some devices receive exactly 16. The 2 devices sharing gx and gy send at most one tile to any one device and exactly 8 tiles to the devices of each gz index. Of one device's tiles at most 4 go to devices of one gz index, and some device reaches that.
All inputs are finite; a program needn't handle non-finite values.
Results may differ from the reference program's by a relative error of at most 0.001.
Values may be sent and summed in bfloat16 or wider, within the bound.
A program may use at most 128 MiB of HBM per device.

```python
import jax
import jax.numpy as jnp
from jax import lax

D = 2048
TILE = 128
TILES_SEQ = 32
TILES_DEV = 8
DEPTH = 2
GROUPS = 16
CAP = 16
TILES = 256
SEQ_LEN = 4096
SEQS = 8


def draw_dest_device(key, part):
    k_amount, k_label, k_column, k_shift = jax.random.split(key, 4)
    half = GROUPS // 2
    amount = jax.random.randint(k_amount, (DEPTH, half), 0, TILES_DEV + 1)
    amount = amount.at[:, 0].set(TILES_DEV)
    loads = jnp.concatenate([TILES_DEV + amount, TILES_DEV - amount], axis=1)
    labels = jax.vmap(lambda k: jax.random.permutation(k, GROUPS))(jax.random.split(k_label, DEPTH))
    columns = jax.vmap(lambda k: jax.random.permutation(k, GROUPS))(jax.random.split(k_column, DEPTH))
    shift = jax.random.randint(k_shift, (GROUPS,), 0, DEPTH)
    ends = jnp.cumsum(loads, axis=1)
    group = jnp.arange(GROUPS)[:, None, None]
    height = jnp.arange(DEPTH)[None, :, None]
    local = jnp.arange(TILES_DEV)[None, None, :]
    within = height * TILES_DEV + local
    target_z = (within + shift[:, None, None]) % DEPTH
    order = within // DEPTH
    column = columns[target_z, group]
    spot = column + GROUPS * order
    label_index = jnp.sum((spot[..., None] >= ends[target_z]).astype(jnp.int32), axis=-1)
    target_group = labels[target_z, label_index]
    return (target_group * DEPTH + target_z).reshape(-1).astype(jnp.int32)


def set_ends(array, rng, low, largest):
    place = [jax.random.randint(jax.random.fold_in(rng, axis), (), 0, length) for axis, length in enumerate(array.shape)]
    longest = array.shape.index(max(array.shape))
    beside = place[:longest] + [(place[longest] + 1) % array.shape[longest]] + place[longest + 1:]
    return array.at[tuple(place)].set(low).at[tuple(beside)].set(largest)


def steps_of(stream_key, dims, cuts, least, largest):
    level = 1.0
    for dim, shards_of in cuts:
        draws = jax.random.uniform(jax.random.fold_in(jax.random.fold_in(stream_key, 6), dim), (shards_of,), jnp.float32, least / len(cuts), largest / len(cuts))
        level = level * jnp.repeat(jnp.exp(draws), dims[dim] // shards_of).reshape((-1,) + (1,) * (len(dims) - 1 - dim))
    return level


def centred(own_key, dims, scale, most, shards=(), kind=jnp.bfloat16):
    result = jax.random.normal(own_key, dims, jnp.float32) * scale
    if len(shards) > 0:
        result = steps_of(own_key, dims, shards, -0.22, 0.18) * result
    return jnp.clip(result, min=-most, max=most).astype(kind)


def setup_inputs(seed: int = 0) -> dict:
    streams_of = jax.random.split(jax.random.key(seed), 6)
    embeds = centred(streams_of[0], (TILES, TILE, D), 1.0, 6.0, ((0, 32),))
    dest_device = draw_dest_device(jax.random.fold_in(streams_of[5], 71), 0)
    shuffle_key = jax.random.permutation(streams_of[2], TILES).astype(jnp.int32)
    lengths = set_ends(jax.random.randint(streams_of[3], (SEQS,), 1, SEQ_LEN + 1), jax.random.fold_in(streams_of[3], 1), 1, SEQ_LEN).astype(jnp.int32)
    gain = jnp.clip(1.0 + 0.18 * jax.random.normal(streams_of[4], (D,), jnp.float32), 0.1, 1.9)
    return {"embeds": embeds, "dest_device": dest_device, "shuffle_key": shuffle_key, "lengths": lengths, "gain": gain}


def normalize(rows, tile_ids, lengths, gain):
    values = rows.astype(jnp.float32)
    meansq = lax.optimization_barrier(jnp.mean(values * values, axis=-1, keepdims=True))
    scaled = values * lax.rsqrt(jnp.maximum(meansq, 0.25)) * gain.astype(jnp.float32)
    limit = lengths[tile_ids // TILES_SEQ]
    position = (tile_ids % TILES_SEQ)[:, None] * TILE + jnp.arange(TILE, dtype=jnp.int32)[None, :]
    keep = position < limit[:, None]
    return jnp.where(keep[:, :, None], scaled, 0.0).astype(jnp.bfloat16)

def reference(embeds, dest_device, shuffle_key, lengths, gain):
    tile_ids = jnp.arange(TILES, dtype=jnp.int32)
    normed = normalize(embeds, tile_ids, lengths, gain)
    same = dest_device[:, None] == dest_device[None, :]
    earlier = shuffle_key[None, :] < shuffle_key[:, None]
    rank = lax.optimization_barrier(jnp.sum((same & earlier).astype(jnp.int32), axis=1)).astype(jnp.int32)
    slots = (dest_device * CAP + rank).astype(jnp.int32)
    packed = jnp.zeros((GROUPS * DEPTH * CAP, TILE, D), jnp.bfloat16)
    return packed.at[slots].set(normed)
```

```python
import functools

import jax
import jax.numpy as jnp
from jax import lax
from jax.experimental import pallas as pl
from jax.experimental.pallas import tpu as pltpu
from jax.sharding import PartitionSpec as P

TILES_SEQ = 32
MESH = pl.DeviceIdType.MESH


def exchange_kernel(
    sizes, first_ref, limit_ref, second_ref, x_ref, gain_ref, recv_ref,
    first, outgoing, y_send, y_recv, g_send, g_recv, own_sem, *arrived,
):
    nx, ny, depth, per_peer, chunks, rows = sizes
    groups = nx * ny
    gx, gy, gz = lax.axis_index("gx"), lax.axis_index("gy"), lax.axis_index("gz")
    group = gx * ny + gy
    offsets = [(dx, dy) for dy in sorted(range(ny), key=lambda d: abs(d - ny // 2)) for dx in range(nx)]
    offsets.remove((0, 0))

    def normed(c, slot):
        tile = first_ref[slot]
        values = x_ref[tile, pl.ds(c * rows, rows), :].astype(jnp.float32)
        meansq = jnp.mean(values * values, axis=-1, keepdims=True)
        scaled = values * lax.rsqrt(jnp.maximum(meansq, 0.25)) * gain_ref[...]
        row = c * rows + lax.broadcasted_iota(jnp.int32, (rows, 1), 0)
        return jnp.where(row < limit_ref[slot], scaled, 0.0).astype(jnp.bfloat16)

    def y_copy(c, dz):
        peer = lax.rem(gz + dz, depth)
        return pltpu.make_async_remote_copy(
            src_ref=first.at[c, dz - 1],
            dst_ref=arrived[c].at[pl.ds(gz * per_peer, per_peer)],
            send_sem=y_send.at[c, dz - 1],
            recv_sem=y_recv.at[c, dz - 1],
            device_id=(gx, gy, peer),
            device_id_type=MESH,
        )

    def y_wait(c, dz):
        origin = lax.rem(gz + depth - dz, depth)
        pltpu.make_async_remote_copy(
            src_ref=first.at[c, dz - 1],
            dst_ref=arrived[c].at[pl.ds(origin * per_peer, per_peer)],
            send_sem=y_send.at[c, dz - 1],
            recv_sem=y_recv.at[c, dz - 1],
            device_id=(gx, gy, origin),
            device_id_type=MESH,
        ).wait_recv()

    def peer_of(k):
        dx, dy = offsets[k]
        return lax.rem(gx + dx, nx), lax.rem(gy + dy, ny)

    def g_copy(c, k):
        px, py = peer_of(k)
        return pltpu.make_async_remote_copy(
            src_ref=outgoing.at[c, k],
            dst_ref=recv_ref.at[c, group],
            send_sem=g_send.at[c, k],
            recv_sem=g_recv.at[c, k],
            device_id=(px, py, gz),
            device_id_type=MESH,
        )

    def own_copy(c):
        return pltpu.make_async_copy(outgoing.at[c, groups - 1], recv_ref.at[c, group], own_sem.at[c])

    def prepare(c):
        for dz in range(1, depth):
            peer = lax.rem(gz + dz, depth)
            for p in range(per_peer):
                first[c, dz - 1, p] = normed(c, peer * per_peer + p)
        for p in range(per_peer):
            arrived[c][gz * per_peer + p] = normed(c, gz * per_peer + p)
        for dz in range(1, depth):
            y_copy(c, dz).start()

    def forward(c):
        for dz in range(1, depth):
            y_wait(c, dz)
        for k in range(groups - 1):
            px, py = peer_of(k)
            outgoing[c, k] = arrived[c][second_ref[px * ny + py]]
        outgoing[c, groups - 1] = arrived[c][second_ref[group]]
        for k in range(groups - 1):
            g_copy(c, k).start()
        own_copy(c).start()

    lead = min(2, chunks)
    for c in range(lead):
        prepare(c)

    for c in range(chunks - lead):
        forward(c)
        prepare(c + lead)

    for c in range(chunks - lead, chunks):
        forward(c)

    for c in range(chunks):
        for dz in range(1, depth):
            y_copy(c, dz).wait_send()

    @pl.loop(0, chunks)
    def _(c):
        for k in range(groups - 1):
            copy = g_copy(c, k)
            copy.wait_send()
            dx, dy = offsets[k]
            sx, sy = lax.rem(gx + nx - dx, nx), lax.rem(gy + ny - dy, ny)
            pltpu.make_async_remote_copy(
                src_ref=outgoing.at[c, k],
                dst_ref=recv_ref.at[c, sx * ny + sy],
                send_sem=g_send.at[c, k],
                recv_sem=g_recv.at[c, k],
                device_id=(sx, sy, gz),
                device_id_type=MESH,
            ).wait_recv()
        own_copy(c).wait()


def place_kernel(source_ref, filled_ref, block_ref, out_ref):
    chunks, _, rows, _ = block_ref.shape
    slot = pl.program_id(0)

    @pl.when(filled_ref[slot] == 1)
    def _():
        for c in range(chunks):
            out_ref[0, pl.ds(c * rows, rows), :] = block_ref[c, 0]

    @pl.when(filled_ref[slot] == 0)
    def _():
        out_ref[...] = jnp.zeros_like(out_ref)


def shards(embeds, dest_device, shuffle_key, lengths, gain):
    tiles_here, tile_rows, width = embeds.shape
    nx, ny, depth = lax.axis_size("gx"), lax.axis_size("gy"), lax.axis_size("gz")
    groups = nx * ny
    group = lax.axis_index("gx") * ny + lax.axis_index("gy")
    gz = lax.axis_index("gz")
    me = group * depth + gz
    per_peer = (tiles_here + depth - 1) // depth
    slots = depth * per_peer
    chunks = 8 if tile_rows % 128 == 0 else 1
    rows = tile_rows // chunks

    both = lax.all_gather(
        jnp.stack([dest_device, shuffle_key]), ("gx", "gy", "gz"), axis=0, tiled=False
    )
    dests = both[:, 0, :]
    keys = both[:, 1, :]
    depths = dests % depth
    order = jnp.arange(tiles_here, dtype=jnp.int32)
    before = (depths[:, None, :] == depths[:, :, None]) & (order[None, None, :] < order[None, :, None])
    spot = jnp.sum(before.astype(jnp.int32), axis=2)

    here_dest = lax.dynamic_slice_in_dim(dests, me, 1, 0)[0]
    here_spot = lax.dynamic_slice_in_dim(spot, me, 1, 0)[0]
    here_slot = here_dest % depth * per_peer + here_spot
    hit = here_slot[None, :] == jnp.arange(slots, dtype=jnp.int32)[:, None]
    first = jnp.sum(jnp.where(hit, order[None, :], 0), axis=1).astype(jnp.int32)
    tile_ids = me * tiles_here + order
    match = (tile_ids // TILES_SEQ)[:, None] == jnp.arange(lengths.shape[0], dtype=jnp.int32)[None, :]
    limit = jnp.sum(jnp.where(match, lengths[None, :], 0), axis=1) - tile_ids % TILES_SEQ * tile_rows
    limits = jnp.sum(jnp.where(hit, jnp.maximum(limit, 0)[None, :], 0), axis=1).astype(jnp.int32)

    by_group_dest = dests.reshape(groups, depth * tiles_here)
    by_group_key = keys.reshape(groups, depth * tiles_here)
    pair_dest = lax.dynamic_slice_in_dim(by_group_dest, group, 1, 0)[0]
    pair_spot = lax.dynamic_slice_in_dim(spot.reshape(groups, depth * tiles_here), group, 1, 0)[0]
    pair_slot = jnp.arange(depth * tiles_here, dtype=jnp.int32) // tiles_here * per_peer + pair_spot
    wanted = jnp.arange(groups, dtype=jnp.int32) * depth + gz
    second = jnp.sum(
        jnp.where(pair_dest[None, :] == wanted[:, None], pair_slot[None, :], 0), axis=1
    ).astype(jnp.int32)

    mine = by_group_dest == me
    key_of = jnp.sum(jnp.where(mine, by_group_key + 1, 0), axis=1)
    valid = key_of > 0
    rank = jnp.sum((valid[None, :] & (key_of[None, :] < key_of[:, None])).astype(jnp.int32), axis=1)
    cap = 2 * tiles_here
    at = valid[None, :] & (rank[None, :] == jnp.arange(cap, dtype=jnp.int32)[:, None])
    source = jnp.sum(jnp.where(at, jnp.arange(groups, dtype=jnp.int32)[None, :], 0), axis=1).astype(jnp.int32)
    filled = jnp.sum(at.astype(jnp.int32), axis=1).astype(jnp.int32)

    smem = pl.BlockSpec(memory_space=pltpu.SMEM)
    vmem = pl.BlockSpec(memory_space=pltpu.VMEM)
    sent = chunks * groups * rows * width * 2
    received = pl.pallas_call(
        functools.partial(exchange_kernel, (nx, ny, depth, per_peer, chunks, rows)),
        out_shape=jax.ShapeDtypeStruct((chunks, groups, rows, width), jnp.bfloat16),
        in_specs=[smem, smem, smem, vmem, vmem],
        out_specs=pl.BlockSpec(memory_space=pl.ANY),
        scratch_shapes=[
            pltpu.VMEM((chunks, depth - 1, per_peer, rows, width), jnp.bfloat16),
            pltpu.VMEM((chunks, groups, rows, width), jnp.bfloat16),
            pltpu.SemaphoreType.DMA((chunks, depth - 1)),
            pltpu.SemaphoreType.DMA((chunks, depth - 1)),
            pltpu.SemaphoreType.DMA((chunks, groups)),
            pltpu.SemaphoreType.DMA((chunks, groups)),
            pltpu.SemaphoreType.DMA((chunks,)),
        ]
        + [pltpu.VMEM((slots, rows, width), jnp.bfloat16)] * chunks,
        compiler_params=pltpu.CompilerParams(
            has_side_effects=True, vmem_limit_bytes=52 * 1024 * 1024
        ),
        name="exchange",
    )(first, limits, second, embeds, gain.reshape(1, width))

    return pl.pallas_call(
        place_kernel,
        grid_spec=pltpu.PrefetchScalarGridSpec(
            num_scalar_prefetch=2,
            grid=(cap,),
            in_specs=[
                pl.BlockSpec((chunks, 1, rows, width), lambda s, source, filled: (0, source[s], 0, 0))
            ],
            out_specs=pl.BlockSpec((1, tile_rows, width), lambda s, source, filled: (s, 0, 0)),
        ),
        out_shape=jax.ShapeDtypeStruct((cap, tile_rows, width), jnp.bfloat16),
        name="place",
    )(source, filled, received)


def solution(mesh):
    return jax.shard_map(
        shards,
        mesh=mesh,
        in_specs=(
            P(("gx", "gy", "gz"), None, None),
            P(("gx", "gy", "gz")),
            P(("gx", "gy", "gz")),
            P(),
            P(),
        ),
        out_specs=P(("gx", "gy", "gz"), None, None),
        check_vma=False,
    )
```

```python
import functools

import jax
import jax.numpy as jnp
from jax import lax
from jax.experimental import pallas as pl
from jax.experimental.pallas import tpu as pltpu
from jax.sharding import PartitionSpec as P

TILES_SEQ = 32
MESH = pl.DeviceIdType.MESH


def exchange_kernel(
    sizes, first_ref, limit_ref, second_ref, x_ref, gain_ref, recv_ref,
    first, outgoing, y_send, y_recv, g_send, g_recv, own_sem, *arrived,
):
    nx, ny, depth, per_peer, chunks, rows = sizes
    groups = nx * ny
    gx, gy, gz = lax.axis_index("gx"), lax.axis_index("gy"), lax.axis_index("gz")
    group = gx * ny + gy
    offsets = [(dx, dy) for dy in sorted(range(ny), key=lambda d: abs(d - ny // 2)) for dx in range(nx)]
    offsets.remove((0, 0))

    def normed(c, slot):
        tile = first_ref[slot]
        values = x_ref[tile, pl.ds(c * rows, rows), :].astype(jnp.float32)
        meansq = jnp.mean(values * values, axis=-1, keepdims=True)
        scaled = values * lax.rsqrt(jnp.maximum(meansq, 0.25)) * gain_ref[...]
        row = c * rows + lax.broadcasted_iota(jnp.int32, (rows, 1), 0)
        return jnp.where(row < limit_ref[slot], scaled, 0.0).astype(jnp.bfloat16)

    def y_copy(c, dz):
        peer = lax.rem(gz + dz, depth)
        return pltpu.make_async_remote_copy(
            src_ref=first.at[c, dz - 1],
            dst_ref=arrived[c].at[pl.ds(gz * per_peer, per_peer)],
            send_sem=y_send.at[c, dz - 1],
            recv_sem=y_recv.at[c, dz - 1],
            device_id=(gx, gy, peer),
            device_id_type=MESH,
        )

    def y_wait(c, dz):
        origin = lax.rem(gz + depth - dz, depth)
        pltpu.make_async_remote_copy(
            src_ref=first.at[c, dz - 1],
            dst_ref=arrived[c].at[pl.ds(origin * per_peer, per_peer)],
            send_sem=y_send.at[c, dz - 1],
            recv_sem=y_recv.at[c, dz - 1],
            device_id=(gx, gy, origin),
            device_id_type=MESH,
        ).wait_recv()

    def peer_of(k):
        dx, dy = offsets[k]
        return lax.rem(gx + dx, nx), lax.rem(gy + dy, ny)

    def g_copy(c, k):
        px, py = peer_of(k)
        return pltpu.make_async_remote_copy(
            src_ref=outgoing.at[c, k],
            dst_ref=recv_ref.at[c, group],
            send_sem=g_send.at[c, k],
            recv_sem=g_recv.at[c, k],
            device_id=(px, py, gz),
            device_id_type=MESH,
        )

    def own_copy(c):
        return pltpu.make_async_copy(outgoing.at[c, groups - 1], recv_ref.at[c, group], own_sem.at[c])

    def prepare(c):
        for dz in range(1, depth):
            peer = lax.rem(gz + dz, depth)
            for p in range(per_peer):
                first[c, dz - 1, p] = normed(c, peer * per_peer + p)
        for p in range(per_peer):
            arrived[c][gz * per_peer + p] = normed(c, gz * per_peer + p)
        for dz in range(1, depth):
            y_copy(c, dz).start()

    def forward(c):
        for dz in range(1, depth):
            y_wait(c, dz)
        for k in range(groups - 1):
            px, py = peer_of(k)
            outgoing[c, k] = arrived[c][second_ref[px * ny + py]]
        outgoing[c, groups - 1] = arrived[c][second_ref[group]]
        for k in range(groups - 1):
            g_copy(c, k).start()
        own_copy(c).start()

    lead = min(2, chunks)
    for c in range(lead):
        prepare(c)

    for c in range(chunks - lead):
        forward(c)
        prepare(c + lead)

    for c in range(chunks - lead, chunks):
        forward(c)

    for c in range(chunks):
        for dz in range(1, depth):
            y_copy(c, dz).wait_send()

    @pl.loop(0, chunks)
    def _(c):
        for k in range(groups - 1):
            copy = g_copy(c, k)
            copy.wait_send()
            dx, dy = offsets[k]
            sx, sy = lax.rem(gx + nx - dx, nx), lax.rem(gy + ny - dy, ny)
            pltpu.make_async_remote_copy(
                src_ref=outgoing.at[c, k],
                dst_ref=recv_ref.at[c, sx * ny + sy],
                send_sem=g_send.at[c, k],
                recv_sem=g_recv.at[c, k],
                device_id=(sx, sy, gz),
                device_id_type=MESH,
            ).wait_recv()
        own_copy(c).wait()


def gather_kernel(sizes, block_ref, all_ref, send_sem, recv_sem, own_sem):
    nx, ny, depth = sizes
    devices = nx * ny * depth
    me = (lax.axis_index("gx") * ny + lax.axis_index("gy")) * depth + lax.axis_index("gz")

    def copy(offset, peer, place):
        return pltpu.make_async_remote_copy(
            src_ref=block_ref,
            dst_ref=all_ref.at[place],
            send_sem=send_sem.at[offset],
            recv_sem=recv_sem.at[offset],
            device_id=(peer // (ny * depth), peer // depth % ny, peer % depth),
            device_id_type=MESH,
        )

    @pl.loop(1, devices)
    def _(offset):
        copy(offset, lax.rem(me + offset, devices), me).start()

    own = pltpu.make_async_copy(block_ref, all_ref.at[me], own_sem)
    own.start()
    own.wait()

    @pl.loop(1, devices)
    def _(offset):
        origin = lax.rem(me + devices - offset, devices)
        copy(offset, origin, origin).wait()


def place_kernel(source_ref, filled_ref, blocks_ref, out_ref, held, zeros, in_sem, out_sem):
    cap = out_ref.shape[0]

    def fetch(slot):
        return pltpu.make_async_copy(blocks_ref.at[:, source_ref[slot]], held.at[slot], in_sem.at[slot])

    def store(slot):
        return pltpu.make_async_copy(held.at[slot], out_ref.at[slot], out_sem.at[slot])

    for slot in range(cap):
        pl.when(filled_ref[slot] == 1)(lambda slot=slot: fetch(slot).start())
    zeros[...] = jnp.zeros_like(zeros)
    for slot in range(cap):

        @pl.when(filled_ref[slot] == 0)
        def _():
            pltpu.make_async_copy(zeros, out_ref.at[slot], out_sem.at[slot]).start()

    for slot in range(cap):

        @pl.when(filled_ref[slot] == 1)
        def _():
            fetch(slot).wait()
            store(slot).start()

    for slot in range(cap):
        store(slot).wait()


def shards(embeds, dest_device, shuffle_key, lengths, gain):
    tiles_here, tile_rows, width = embeds.shape
    nx, ny, depth = lax.axis_size("gx"), lax.axis_size("gy"), lax.axis_size("gz")
    groups = nx * ny
    group = lax.axis_index("gx") * ny + lax.axis_index("gy")
    gz = lax.axis_index("gz")
    me = group * depth + gz
    per_peer = (tiles_here + depth - 1) // depth
    slots = depth * per_peer
    chunks = 8 if tile_rows % 128 == 0 else 1
    rows = tile_rows // chunks

    smem = pl.BlockSpec(memory_space=pltpu.SMEM)
    vmem = pl.BlockSpec(memory_space=pltpu.VMEM)
    hbm = pl.BlockSpec(memory_space=pl.ANY)
    devices = groups * depth
    lanes = -(-2 * tiles_here // 128) * 128
    block = jnp.pad(jnp.concatenate([dest_device, shuffle_key])[None, :], ((0, 0), (0, lanes - 2 * tiles_here)))
    both = pl.pallas_call(
        functools.partial(gather_kernel, (nx, ny, depth)),
        out_shape=jax.ShapeDtypeStruct((devices, 1, lanes), jnp.int32),
        in_specs=[vmem],
        out_specs=vmem,
        scratch_shapes=[
            pltpu.SemaphoreType.DMA((devices,)),
            pltpu.SemaphoreType.DMA((devices,)),
            pltpu.SemaphoreType.DMA,
        ],
        compiler_params=pltpu.CompilerParams(has_side_effects=True),
        name="gather_tables",
    )(block)
    dests = both[:, 0, :tiles_here]
    keys = both[:, 0, tiles_here : 2 * tiles_here]
    depths = dests % depth
    order = jnp.arange(tiles_here, dtype=jnp.int32)
    before = (depths[:, None, :] == depths[:, :, None]) & (order[None, None, :] < order[None, :, None])
    spot = jnp.sum(before.astype(jnp.int32), axis=2)

    here_dest = lax.dynamic_slice_in_dim(dests, me, 1, 0)[0]
    here_spot = lax.dynamic_slice_in_dim(spot, me, 1, 0)[0]
    here_slot = here_dest % depth * per_peer + here_spot
    hit = here_slot[None, :] == jnp.arange(slots, dtype=jnp.int32)[:, None]
    first = jnp.sum(jnp.where(hit, order[None, :], 0), axis=1).astype(jnp.int32)
    tile_ids = me * tiles_here + order
    match = (tile_ids // TILES_SEQ)[:, None] == jnp.arange(lengths.shape[0], dtype=jnp.int32)[None, :]
    limit = jnp.sum(jnp.where(match, lengths[None, :], 0), axis=1) - tile_ids % TILES_SEQ * tile_rows
    limits = jnp.sum(jnp.where(hit, jnp.maximum(limit, 0)[None, :], 0), axis=1).astype(jnp.int32)

    by_group_dest = dests.reshape(groups, depth * tiles_here)
    by_group_key = keys.reshape(groups, depth * tiles_here)
    pair_dest = lax.dynamic_slice_in_dim(by_group_dest, group, 1, 0)[0]
    pair_spot = lax.dynamic_slice_in_dim(spot.reshape(groups, depth * tiles_here), group, 1, 0)[0]
    pair_slot = jnp.arange(depth * tiles_here, dtype=jnp.int32) // tiles_here * per_peer + pair_spot
    wanted = jnp.arange(groups, dtype=jnp.int32) * depth + gz
    second = jnp.sum(
        jnp.where(pair_dest[None, :] == wanted[:, None], pair_slot[None, :], 0), axis=1
    ).astype(jnp.int32)

    mine = by_group_dest == me
    key_of = jnp.sum(jnp.where(mine, by_group_key + 1, 0), axis=1)
    valid = key_of > 0
    rank = jnp.sum((valid[None, :] & (key_of[None, :] < key_of[:, None])).astype(jnp.int32), axis=1)
    cap = 2 * tiles_here
    at = valid[None, :] & (rank[None, :] == jnp.arange(cap, dtype=jnp.int32)[:, None])
    source = jnp.sum(jnp.where(at, jnp.arange(groups, dtype=jnp.int32)[None, :], 0), axis=1).astype(jnp.int32)
    filled = jnp.sum(at.astype(jnp.int32), axis=1).astype(jnp.int32)

    received = pl.pallas_call(
        functools.partial(exchange_kernel, (nx, ny, depth, per_peer, chunks, rows)),
        out_shape=jax.ShapeDtypeStruct((chunks, groups, rows, width), jnp.bfloat16),
        in_specs=[smem, smem, smem, vmem, vmem],
        out_specs=hbm,
        scratch_shapes=[
            pltpu.VMEM((chunks, depth - 1, per_peer, rows, width), jnp.bfloat16),
            pltpu.VMEM((chunks, groups, rows, width), jnp.bfloat16),
            pltpu.SemaphoreType.DMA((chunks, depth - 1)),
            pltpu.SemaphoreType.DMA((chunks, depth - 1)),
            pltpu.SemaphoreType.DMA((chunks, groups)),
            pltpu.SemaphoreType.DMA((chunks, groups)),
            pltpu.SemaphoreType.DMA((chunks,)),
        ]
        + [pltpu.VMEM((slots, rows, width), jnp.bfloat16)] * chunks,
        compiler_params=pltpu.CompilerParams(
            has_side_effects=True, vmem_limit_bytes=52 * 1024 * 1024
        ),
        name="exchange",
    )(first, limits, second, embeds, gain.reshape(1, width))

    packed = pl.pallas_call(
        place_kernel,
        out_shape=jax.ShapeDtypeStruct((cap, chunks, rows, width), jnp.bfloat16),
        in_specs=[smem, smem, hbm],
        out_specs=hbm,
        scratch_shapes=[
            pltpu.VMEM((cap, chunks, rows, width), jnp.bfloat16),
            pltpu.VMEM((chunks, rows, width), jnp.bfloat16),
            pltpu.SemaphoreType.DMA((cap,)),
            pltpu.SemaphoreType.DMA((cap,)),
        ],
        compiler_params=pltpu.CompilerParams(vmem_limit_bytes=52 * 1024 * 1024),
        name="place",
    )(source, filled, received)
    return packed.reshape(cap, tile_rows, width)


def solution(mesh):
    return jax.shard_map(
        shards,
        mesh=mesh,
        in_specs=(
            P(("gx", "gy", "gz"), None, None),
            P(("gx", "gy", "gz")),
            P(("gx", "gy", "gz")),
            P(),
            P(),
        ),
        out_specs=P(("gx", "gy", "gz"), None, None),
        check_vma=False,
    )
```

```python
import functools

import jax
import jax.numpy as jnp
from jax import lax
from jax.experimental import pallas as pl
from jax.experimental.pallas import tpu as pltpu
from jax.sharding import PartitionSpec as P

TILES_SEQ = 32
MESH = pl.DeviceIdType.MESH


def exchange_kernel(
    sizes, first_ref, limit_ref, note_ref, x_ref, gain_ref, recv_ref, keys_ref,
    first, outgoing, notes, note_table, second, keys_out, y_send, y_recv, g_send, g_recv, own_sem,
    note_send, note_recv, note_sem, key_send, key_recv, *arrived,
):
    nx, ny, depth, per_peer, chunks, rows = sizes
    groups = nx * ny
    gx, gy, gz = lax.axis_index("gx"), lax.axis_index("gy"), lax.axis_index("gz")
    group = gx * ny + gy
    offsets = [(dx, dy) for dy in sorted(range(ny), key=lambda d: abs(d - ny // 2)) for dx in range(nx)]
    offsets.remove((0, 0))

    def normed(c, slot):
        tile = first_ref[slot]
        values = x_ref[tile, pl.ds(c * rows, rows), :].astype(jnp.float32)
        meansq = jnp.mean(values * values, axis=-1, keepdims=True)
        scaled = values * lax.rsqrt(jnp.maximum(meansq, 0.25)) * gain_ref[...]
        row = c * rows + lax.broadcasted_iota(jnp.int32, (rows, 1), 0)
        return jnp.where(row < limit_ref[slot], scaled, 0.0).astype(jnp.bfloat16)

    def y_copy(c, dz):
        peer = lax.rem(gz + dz, depth)
        return pltpu.make_async_remote_copy(
            src_ref=first.at[c, dz - 1],
            dst_ref=arrived[c].at[pl.ds(gz * per_peer, per_peer)],
            send_sem=y_send.at[c, dz - 1],
            recv_sem=y_recv.at[c, dz - 1],
            device_id=(gx, gy, peer),
            device_id_type=MESH,
        )

    def y_wait(c, dz):
        origin = lax.rem(gz + depth - dz, depth)
        pltpu.make_async_remote_copy(
            src_ref=first.at[c, dz - 1],
            dst_ref=arrived[c].at[pl.ds(origin * per_peer, per_peer)],
            send_sem=y_send.at[c, dz - 1],
            recv_sem=y_recv.at[c, dz - 1],
            device_id=(gx, gy, origin),
            device_id_type=MESH,
        ).wait_recv()

    def peer_of(k):
        dx, dy = offsets[k]
        return lax.rem(gx + dx, nx), lax.rem(gy + dy, ny)

    def g_copy(c, k):
        px, py = peer_of(k)
        return pltpu.make_async_remote_copy(
            src_ref=outgoing.at[c, k],
            dst_ref=recv_ref.at[c, group],
            send_sem=g_send.at[c, k],
            recv_sem=g_recv.at[c, k],
            device_id=(px, py, gz),
            device_id_type=MESH,
        )

    def own_copy(c):
        return pltpu.make_async_copy(outgoing.at[c, groups - 1], recv_ref.at[c, group], own_sem.at[c])

    def note_copy(dz, peer, place):
        return pltpu.make_async_remote_copy(
            src_ref=note_ref.at[peer],
            dst_ref=notes.at[place],
            send_sem=note_send.at[dz - 1],
            recv_sem=note_recv.at[dz - 1],
            device_id=(gx, gy, peer),
            device_id_type=MESH,
        )

    def key_copy(k, px, py, place):
        return pltpu.make_async_remote_copy(
            src_ref=keys_out.at[k],
            dst_ref=keys_ref.at[place],
            send_sem=key_send.at[k],
            recv_sem=key_recv.at[k],
            device_id=(px, py, gz),
            device_id_type=MESH,
        )

    def prepare(c):
        for dz in range(1, depth):
            peer = lax.rem(gz + dz, depth)
            for p in range(per_peer):
                first[c, dz - 1, p] = normed(c, peer * per_peer + p)
        for p in range(per_peer):
            arrived[c][gz * per_peer + p] = normed(c, gz * per_peer + p)

    def send_first(c):
        for dz in range(1, depth):
            y_copy(c, dz).start()

    def find_slots():
        for dz in range(1, depth):
            origin = lax.rem(gz + depth - dz, depth)
            note_copy(dz, origin, origin).wait()
        tables = [
            pltpu.make_async_copy(
                notes.at[lax.rem(gz + dz, depth)], note_table.at[lax.rem(gz + dz, depth)], note_sem.at[dz]
            )
            for dz in range(1, depth)
        ]
        tables.append(pltpu.make_async_copy(note_ref.at[gz], note_table.at[gz], note_sem.at[0]))
        for copy in tables:
            copy.start()
        for copy in tables:
            copy.wait()

        for k in range(groups):
            px, py = peer_of(k) if k < groups - 1 else (gx, gy)
            wanted = px * ny + py
            slot, key = jnp.int32(0), jnp.int32(0)
            for z in range(depth):
                for p in range(per_peer):
                    hit = note_table[z, 0, p] == wanted
                    slot = jnp.where(hit, z * per_peer + p, slot)
                    key = jnp.where(hit, note_table[z, 0, per_peer + p], key)
            second[k] = slot
            row = jnp.full(keys_out.shape[1:], key, jnp.int32)
            if k < groups - 1:
                keys_out[k] = row
            else:
                keys_ref[group] = row

    def forward(c):
        for dz in range(1, depth):
            y_wait(c, dz)
        for k in range(groups):
            outgoing[c, k] = arrived[c][second[k]]
        for k in range(groups - 1):
            g_copy(c, k).start()
        own_copy(c).start()

    barrier = pltpu.get_barrier_semaphore()
    for dz in range(1, depth):
        pl.semaphore_signal(
            barrier, inc=1, device_id=(gx, gy, lax.rem(gz + dz, depth)), device_id_type=MESH
        )
    for k in range(groups - 1):
        px, py = peer_of(k)
        pl.semaphore_signal(barrier, inc=1, device_id=(px, py, gz), device_id_type=MESH)
    prepare(0)
    pl.semaphore_wait(barrier, depth - 1 + groups - 1)
    for dz in range(1, depth):
        note_copy(dz, lax.rem(gz + dz, depth), gz).start()
    send_first(0)
    if chunks > 1:
        prepare(1)
        send_first(1)
    find_slots()
    forward(0)
    for k in range(groups - 1):
        px, py = peer_of(k)
        key_copy(k, px, py, group).start()
    for c in range(2, chunks):
        prepare(c)
        send_first(c)
        forward(c - 1)
    if chunks > 1:
        forward(chunks - 1)

    for c in range(chunks):
        for dz in range(1, depth):
            y_copy(c, dz).wait_send()
    sources = []
    for dx, dy in offsets:
        sources.append((lax.rem(gx + nx - dx, nx), lax.rem(gy + ny - dy, ny)))
    for k, (sx, sy) in enumerate(sources):
        key_copy(k, sx, sy, sx * ny + sy).wait()

    @pl.loop(0, chunks)
    def _(c):
        for k, (sx, sy) in enumerate(sources):
            g_copy(c, k).wait_send()
            pltpu.make_async_remote_copy(
                src_ref=outgoing.at[c, k],
                dst_ref=recv_ref.at[c, sx * ny + sy],
                send_sem=g_send.at[c, k],
                recv_sem=g_recv.at[c, k],
                device_id=(sx, sy, gz),
                device_id_type=MESH,
            ).wait_recv()
        own_copy(c).wait()


def place_kernel(source_ref, filled_ref, blocks_ref, out_ref, held, zeros, in_sem, out_sem):
    cap = out_ref.shape[0]

    def fetch(slot):
        return pltpu.make_async_copy(blocks_ref.at[:, source_ref[slot]], held.at[slot], in_sem.at[slot])

    def store(slot):
        return pltpu.make_async_copy(held.at[slot], out_ref.at[slot], out_sem.at[slot])

    for slot in range(cap):
        pl.when(filled_ref[slot] == 1)(lambda slot=slot: fetch(slot).start())
    zeros[...] = jnp.zeros_like(zeros)
    for slot in range(cap):

        @pl.when(filled_ref[slot] == 0)
        def _():
            pltpu.make_async_copy(zeros, out_ref.at[slot], out_sem.at[slot]).start()

    for slot in range(cap):

        @pl.when(filled_ref[slot] == 1)
        def _():
            fetch(slot).wait()
            store(slot).start()

    for slot in range(cap):
        store(slot).wait()


def shards(embeds, dest_device, shuffle_key, lengths, gain):
    tiles_here, tile_rows, width = embeds.shape
    nx, ny, depth = lax.axis_size("gx"), lax.axis_size("gy"), lax.axis_size("gz")
    groups = nx * ny
    group = lax.axis_index("gx") * ny + lax.axis_index("gy")
    gz = lax.axis_index("gz")
    me = group * depth + gz
    per_peer = (tiles_here + depth - 1) // depth
    slots = depth * per_peer
    chunks = 8 if tile_rows % 128 == 0 else 1
    rows = tile_rows // chunks

    smem = pl.BlockSpec(memory_space=pltpu.SMEM)
    vmem = pl.BlockSpec(memory_space=pltpu.VMEM)
    hbm = pl.BlockSpec(memory_space=pl.ANY)
    order = jnp.arange(tiles_here, dtype=jnp.int32)
    depths = dest_device % depth
    before = (depths[None, :] == depths[:, None]) & (order[None, :] < order[:, None])
    spot = jnp.sum(before.astype(jnp.int32), axis=1)
    here_slot = depths * per_peer + spot
    hit = here_slot[None, :] == jnp.arange(slots, dtype=jnp.int32)[:, None]
    tile_ids = me * tiles_here + order
    match = (tile_ids // TILES_SEQ)[:, None] == jnp.arange(lengths.shape[0], dtype=jnp.int32)[None, :]
    limit = jnp.sum(jnp.where(match, lengths[None, :], 0), axis=1) - tile_ids % TILES_SEQ * tile_rows
    first = jnp.sum(jnp.where(hit, order[None, :], 0), axis=1).astype(jnp.int32)
    limits = jnp.sum(jnp.where(hit, jnp.maximum(limit, 0)[None, :], 0), axis=1).astype(jnp.int32)
    slot_group = jnp.sum(jnp.where(hit, dest_device[None, :] // depth + 1, 0), axis=1) - 1
    slot_key = jnp.sum(jnp.where(hit, shuffle_key[None, :] + 1, 0), axis=1)
    lanes = -(-2 * per_peer // 128) * 128
    note = jnp.concatenate([slot_group.reshape(depth, per_peer), slot_key.reshape(depth, per_peer)], axis=1)
    note = jnp.pad(note.astype(jnp.int32), ((0, 0), (0, lanes - 2 * per_peer)))[:, None, :]

    received, key_rows = pl.pallas_call(
        functools.partial(exchange_kernel, (nx, ny, depth, per_peer, chunks, rows)),
        out_shape=(
            jax.ShapeDtypeStruct((chunks, groups, rows, width), jnp.bfloat16),
            jax.ShapeDtypeStruct((groups, 1, 128), jnp.int32),
        ),
        in_specs=[smem, smem, vmem, vmem, vmem],
        out_specs=(hbm, vmem),
        scratch_shapes=[
            pltpu.VMEM((chunks, depth - 1, per_peer, rows, width), jnp.bfloat16),
            pltpu.VMEM((chunks, groups, rows, width), jnp.bfloat16),
            pltpu.VMEM((depth, 1, lanes), jnp.int32),
            pltpu.SMEM((depth, 1, lanes), jnp.int32),
            pltpu.SMEM((groups,), jnp.int32),
            pltpu.VMEM((groups, 1, 128), jnp.int32),
            pltpu.SemaphoreType.DMA((chunks, depth - 1)),
            pltpu.SemaphoreType.DMA((chunks, depth - 1)),
            pltpu.SemaphoreType.DMA((chunks, groups)),
            pltpu.SemaphoreType.DMA((chunks, groups)),
            pltpu.SemaphoreType.DMA((chunks,)),
            pltpu.SemaphoreType.DMA((depth,)),
            pltpu.SemaphoreType.DMA((depth,)),
            pltpu.SemaphoreType.DMA((depth,)),
            pltpu.SemaphoreType.DMA((groups,)),
            pltpu.SemaphoreType.DMA((groups,)),
        ]
        + [pltpu.VMEM((slots, rows, width), jnp.bfloat16)] * chunks,
        compiler_params=pltpu.CompilerParams(
            collective_id=0, has_side_effects=True, vmem_limit_bytes=52 * 1024 * 1024
        ),
        name="exchange",
    )(first, limits, note, embeds, gain.reshape(1, width))

    key_of = key_rows[:, 0, 0]
    valid = key_of > 0
    rank = jnp.sum((valid[None, :] & (key_of[None, :] < key_of[:, None])).astype(jnp.int32), axis=1)
    cap = 2 * tiles_here
    at = valid[None, :] & (rank[None, :] == jnp.arange(cap, dtype=jnp.int32)[:, None])
    source = jnp.sum(jnp.where(at, jnp.arange(groups, dtype=jnp.int32)[None, :], 0), axis=1).astype(jnp.int32)
    filled = jnp.sum(at.astype(jnp.int32), axis=1).astype(jnp.int32)

    packed = pl.pallas_call(
        place_kernel,
        out_shape=jax.ShapeDtypeStruct((cap, chunks, rows, width), jnp.bfloat16),
        in_specs=[smem, smem, hbm],
        out_specs=hbm,
        scratch_shapes=[
            pltpu.VMEM((cap, chunks, rows, width), jnp.bfloat16),
            pltpu.VMEM((chunks, rows, width), jnp.bfloat16),
            pltpu.SemaphoreType.DMA((cap,)),
            pltpu.SemaphoreType.DMA((cap,)),
        ],
        compiler_params=pltpu.CompilerParams(vmem_limit_bytes=52 * 1024 * 1024),
        name="place",
    )(source, filled, received)
    return packed.reshape(cap, tile_rows, width)


def solution(mesh):
    return jax.shard_map(
        shards,
        mesh=mesh,
        in_specs=(
            P(("gx", "gy", "gz"), None, None),
            P(("gx", "gy", "gz")),
            P(("gx", "gy", "gz")),
            P(),
            P(),
        ),
        out_specs=P(("gx", "gy", "gz"), None, None),
        check_vma=False,
    )
```

```python
import functools

import jax
import jax.numpy as jnp
from jax import lax
from jax.experimental import pallas as pl
from jax.experimental.pallas import tpu as pltpu
from jax.sharding import PartitionSpec as P

TILES_SEQ = 32
MESH = pl.DeviceIdType.MESH


def exchange_kernel(
    sizes, dest_ref, order_ref, length_ref, x_ref, gain_ref, recv_ref, keys_ref,
    gain, first_table, limit_table, note_out, notes, note_table, second, keys_out,
    x_sem, gain_sem, y_send, y_recv, g_send, g_recv, own_sem,
    note_send, note_recv, note_sem, key_send, key_recv, *buffers,
):
    nx, ny, depth, per_peer, chunk_rows = sizes
    chunks = len(chunk_rows)
    starts = [sum(chunk_rows[:c]) for c in range(chunks)]
    groups = nx * ny
    tiles_here, tile_rows, _ = x_ref.shape
    raw, first, arrived, outgoing = (buffers[i * chunks : (i + 1) * chunks] for i in range(4))
    gx, gy, gz = lax.axis_index("gx"), lax.axis_index("gy"), lax.axis_index("gz")
    group = gx * ny + gy
    me = group * depth + gz
    offsets = [(dx, dy) for dy in sorted(range(ny), key=lambda d: abs(d - ny // 2)) for dx in range(nx)]
    offsets.remove((0, 0))

    def load(c):
        return pltpu.make_async_copy(
            x_ref.at[:, pl.ds(starts[c], chunk_rows[c])], raw[c], x_sem.at[c]
        )

    def fill_tables():
        depths = [lax.rem(dest_ref[i], depth) for i in range(tiles_here)]
        dest_groups = [lax.div(dest_ref[i], depth) for i in range(tiles_here)]
        places, limits = [], []
        for i in range(tiles_here):
            spot = jnp.int32(0)
            for j in range(i):
                spot = spot + jnp.where(depths[j] == depths[i], 1, 0)
            places.append(depths[i] * per_peer + spot)
            tile = me * tiles_here + i
            length = length_ref[tile // TILES_SEQ]
            limits.append(jnp.maximum(length - tile % TILES_SEQ * tile_rows, 0))
        lane = lax.broadcasted_iota(jnp.int32, note_out.shape[1:], 1)
        for z in range(depth):
            row = jnp.zeros(note_out.shape[1:], jnp.int32)
            for p in range(per_peer):
                slot = z * per_peer + p
                tile, limit, dest_group, key = (jnp.int32(v) for v in (0, 0, -1, 0))
                for i in range(tiles_here):
                    hit = places[i] == slot
                    tile = jnp.where(hit, i, tile)
                    limit = jnp.where(hit, limits[i], limit)
                    dest_group = jnp.where(hit, dest_groups[i], dest_group)
                    key = jnp.where(hit, order_ref[i] + 1, key)
                first_table[slot] = tile
                limit_table[slot] = limit
                row = jnp.where(lane == p, dest_group, row)
                row = jnp.where(lane == per_peer + p, key, row)
            note_out[z] = row

    def normed(c, slot):
        rows = chunk_rows[c]
        values = raw[c][first_table[slot]].astype(jnp.float32)
        meansq = jnp.mean(values * values, axis=-1, keepdims=True)
        scaled = values * lax.rsqrt(jnp.maximum(meansq, 0.25)) * gain[...]
        row = starts[c] + lax.broadcasted_iota(jnp.int32, (rows, 1), 0)
        return jnp.where(row < limit_table[slot], scaled, 0.0).astype(jnp.bfloat16)

    def y_copy(c, dz, peer, origin):
        return pltpu.make_async_remote_copy(
            src_ref=first[c].at[dz - 1],
            dst_ref=arrived[c].at[pl.ds(origin * per_peer, per_peer)],
            send_sem=y_send.at[c, dz - 1],
            recv_sem=y_recv.at[c, dz - 1],
            device_id=(gx, gy, peer),
            device_id_type=MESH,
        )

    def peer_of(k):
        dx, dy = offsets[k]
        return lax.rem(gx + dx, nx), lax.rem(gy + dy, ny)

    def g_copy(c, k, px, py, origin):
        return pltpu.make_async_remote_copy(
            src_ref=outgoing[c].at[k],
            dst_ref=recv_ref.at[origin, pl.ds(starts[c], chunk_rows[c])],
            send_sem=g_send.at[c, k],
            recv_sem=g_recv.at[c, k],
            device_id=(px, py, gz),
            device_id_type=MESH,
        )

    def own_copy(c):
        return pltpu.make_async_copy(
            outgoing[c].at[groups - 1],
            recv_ref.at[group, pl.ds(starts[c], chunk_rows[c])],
            own_sem.at[c],
        )

    def note_copy(dz, peer, place):
        return pltpu.make_async_remote_copy(
            src_ref=note_out.at[peer],
            dst_ref=notes.at[place],
            send_sem=note_send.at[dz - 1],
            recv_sem=note_recv.at[dz - 1],
            device_id=(gx, gy, peer),
            device_id_type=MESH,
        )

    def key_copy(k, px, py, place):
        return pltpu.make_async_remote_copy(
            src_ref=keys_out.at[k],
            dst_ref=keys_ref.at[place],
            send_sem=key_send.at[k],
            recv_sem=key_recv.at[k],
            device_id=(px, py, gz),
            device_id_type=MESH,
        )

    def prepare(c):
        load(c).wait()
        for dz in range(1, depth):
            peer = lax.rem(gz + dz, depth)
            for p in range(per_peer):
                first[c][dz - 1, p] = normed(c, peer * per_peer + p)
        for p in range(per_peer):
            arrived[c][gz * per_peer + p] = normed(c, gz * per_peer + p)

    def send_first(c):
        for dz in range(1, depth):
            y_copy(c, dz, lax.rem(gz + dz, depth), gz).start()

    def find_slots():
        for dz in range(1, depth):
            origin = lax.rem(gz + depth - dz, depth)
            note_copy(dz, origin, origin).wait()
        tables = [
            pltpu.make_async_copy(
                notes.at[lax.rem(gz + dz, depth)], note_table.at[lax.rem(gz + dz, depth)], note_sem.at[dz]
            )
            for dz in range(1, depth)
        ]
        tables.append(pltpu.make_async_copy(note_out.at[gz], note_table.at[gz], note_sem.at[0]))
        for copy in tables:
            copy.start()
        for copy in tables:
            copy.wait()

        for k in range(groups):
            px, py = peer_of(k) if k < groups - 1 else (gx, gy)
            wanted = px * ny + py
            slot, key = jnp.int32(0), jnp.int32(0)
            for z in range(depth):
                for p in range(per_peer):
                    hit = note_table[z, 0, p] == wanted
                    slot = jnp.where(hit, z * per_peer + p, slot)
                    key = jnp.where(hit, note_table[z, 0, per_peer + p], key)
            second[k] = slot
            row = jnp.full(keys_out.shape[1:], key, jnp.int32)
            if k < groups - 1:
                keys_out[k] = row
            else:
                keys_ref[group] = row

    def forward(c):
        for dz in range(1, depth):
            origin = lax.rem(gz + depth - dz, depth)
            y_copy(c, dz, origin, origin).wait_recv()
        for k in range(groups):
            outgoing[c][k] = arrived[c][second[k]]
        for k in range(groups - 1):
            px, py = peer_of(k)
            g_copy(c, k, px, py, group).start()
        own_copy(c).start()

    gain_copy = pltpu.make_async_copy(gain_ref, gain, gain_sem)
    gain_copy.start()
    for c in range(chunks):
        load(c).start()
    barrier = pltpu.get_barrier_semaphore()
    for dz in range(1, depth):
        pl.semaphore_signal(
            barrier, inc=1, device_id=(gx, gy, lax.rem(gz + dz, depth)), device_id_type=MESH
        )
    for k in range(groups - 1):
        px, py = peer_of(k)
        pl.semaphore_signal(barrier, inc=1, device_id=(px, py, gz), device_id_type=MESH)
    fill_tables()
    gain_copy.wait()
    prepare(0)
    pl.semaphore_wait(barrier, depth - 1 + groups - 1)
    for dz in range(1, depth):
        note_copy(dz, lax.rem(gz + dz, depth), gz).start()
    send_first(0)
    if chunks > 1:
        prepare(1)
        send_first(1)
    find_slots()
    forward(0)
    for k in range(groups - 1):
        px, py = peer_of(k)
        key_copy(k, px, py, group).start()
    for c in range(2, chunks):
        prepare(c)
        send_first(c)
        forward(c - 1)
    if chunks > 1:
        forward(chunks - 1)

    for c in range(chunks):
        for dz in range(1, depth):
            y_copy(c, dz, lax.rem(gz + dz, depth), gz).wait_send()
    sources = []
    for dx, dy in offsets:
        sources.append((lax.rem(gx + nx - dx, nx), lax.rem(gy + ny - dy, ny)))
    for k, (sx, sy) in enumerate(sources):
        key_copy(k, sx, sy, sx * ny + sy).wait()
    for c in range(chunks):
        for k, (sx, sy) in enumerate(sources):
            g_copy(c, k, sx, sy, sx * ny + sy).wait()
        own_copy(c).wait()


def place_kernel(source_ref, filled_ref, blocks_ref, out_ref, held, zeros, in_sem, out_sem):
    cap = out_ref.shape[0]

    def fetch(slot):
        return pltpu.make_async_copy(blocks_ref.at[source_ref[slot]], held.at[slot], in_sem.at[slot])

    def store(slot):
        return pltpu.make_async_copy(held.at[slot], out_ref.at[slot], out_sem.at[slot])

    for slot in range(cap):
        pl.when(filled_ref[slot] == 1)(lambda slot=slot: fetch(slot).start())
    zeros[...] = jnp.zeros_like(zeros)
    for slot in range(cap):

        @pl.when(filled_ref[slot] == 0)
        def _():
            pltpu.make_async_copy(zeros, out_ref.at[slot], out_sem.at[slot]).start()

    for slot in range(cap):

        @pl.when(filled_ref[slot] == 1)
        def _():
            fetch(slot).wait()
            store(slot).start()

    for slot in range(cap):
        store(slot).wait()


def shards(embeds, dest_device, shuffle_key, lengths, gain):
    tiles_here, tile_rows, width = embeds.shape
    nx, ny, depth = lax.axis_size("gx"), lax.axis_size("gy"), lax.axis_size("gz")
    groups = nx * ny
    per_peer = (tiles_here + depth - 1) // depth
    slots = depth * per_peer
    chunk_rows = (tile_rows,)
    if tile_rows % 128 == 0:
        chunk_rows = tuple(part * tile_rows // 16 for part in (1, 1, 2, 2, 4, 4, 2))
    chunks = len(chunk_rows)

    smem = pl.BlockSpec(memory_space=pltpu.SMEM)
    vmem = pl.BlockSpec(memory_space=pltpu.VMEM)
    hbm = pl.BlockSpec(memory_space=pl.ANY)
    lanes = -(-2 * per_peer // 128) * 128
    received, key_rows = pl.pallas_call(
        functools.partial(exchange_kernel, (nx, ny, depth, per_peer, chunk_rows)),
        out_shape=(
            jax.ShapeDtypeStruct((groups, tile_rows, width), jnp.bfloat16),
            jax.ShapeDtypeStruct((groups, 1, 128), jnp.int32),
        ),
        in_specs=[smem, smem, smem, hbm, hbm],
        out_specs=(hbm, vmem),
        scratch_shapes=[
            pltpu.VMEM((1, width), jnp.float32),
            pltpu.SMEM((slots,), jnp.int32),
            pltpu.SMEM((slots,), jnp.int32),
            pltpu.VMEM((depth, 1, lanes), jnp.int32),
            pltpu.VMEM((depth, 1, lanes), jnp.int32),
            pltpu.SMEM((depth, 1, lanes), jnp.int32),
            pltpu.SMEM((groups,), jnp.int32),
            pltpu.VMEM((groups, 1, 128), jnp.int32),
            pltpu.SemaphoreType.DMA((chunks,)),
            pltpu.SemaphoreType.DMA,
            pltpu.SemaphoreType.DMA((chunks, depth - 1)),
            pltpu.SemaphoreType.DMA((chunks, depth - 1)),
            pltpu.SemaphoreType.DMA((chunks, groups)),
            pltpu.SemaphoreType.DMA((chunks, groups)),
            pltpu.SemaphoreType.DMA((chunks,)),
            pltpu.SemaphoreType.DMA((depth,)),
            pltpu.SemaphoreType.DMA((depth,)),
            pltpu.SemaphoreType.DMA((depth,)),
            pltpu.SemaphoreType.DMA((groups,)),
            pltpu.SemaphoreType.DMA((groups,)),
        ]
        + [pltpu.VMEM((tiles_here, rows, width), jnp.bfloat16) for rows in chunk_rows]
        + [pltpu.VMEM((depth - 1, per_peer, rows, width), jnp.bfloat16) for rows in chunk_rows]
        + [pltpu.VMEM((slots, rows, width), jnp.bfloat16) for rows in chunk_rows]
        + [pltpu.VMEM((groups, rows, width), jnp.bfloat16) for rows in chunk_rows],
        compiler_params=pltpu.CompilerParams(
            collective_id=0, has_side_effects=True, vmem_limit_bytes=52 * 1024 * 1024
        ),
        name="exchange",
    )(dest_device, shuffle_key, lengths, embeds, gain.reshape(1, width))

    key_of = key_rows[:, 0, 0]
    valid = key_of > 0
    rank = jnp.sum((valid[None, :] & (key_of[None, :] < key_of[:, None])).astype(jnp.int32), axis=1)
    cap = 2 * tiles_here
    at = valid[None, :] & (rank[None, :] == jnp.arange(cap, dtype=jnp.int32)[:, None])
    source = jnp.sum(jnp.where(at, jnp.arange(groups, dtype=jnp.int32)[None, :], 0), axis=1).astype(jnp.int32)
    filled = jnp.sum(at.astype(jnp.int32), axis=1).astype(jnp.int32)

    return pl.pallas_call(
        place_kernel,
        out_shape=jax.ShapeDtypeStruct((cap, tile_rows, width), jnp.bfloat16),
        in_specs=[smem, smem, hbm],
        out_specs=hbm,
        scratch_shapes=[
            pltpu.VMEM((cap, tile_rows, width), jnp.bfloat16),
            pltpu.VMEM((tile_rows, width), jnp.bfloat16),
            pltpu.SemaphoreType.DMA((cap,)),
            pltpu.SemaphoreType.DMA((cap,)),
        ],
        compiler_params=pltpu.CompilerParams(vmem_limit_bytes=52 * 1024 * 1024),
        name="place",
    )(source, filled, received)


def solution(mesh):
    return jax.shard_map(
        shards,
        mesh=mesh,
        in_specs=(
            P(("gx", "gy", "gz"), None, None),
            P(("gx", "gy", "gz")),
            P(("gx", "gy", "gz")),
            P(),
            P(),
        ),
        out_specs=P(("gx", "gy", "gz"), None, None),
        check_vma=False,
    )
```

```python
import functools

import jax
import jax.numpy as jnp
from jax import lax
from jax.experimental import pallas as pl
from jax.experimental.pallas import tpu as pltpu
from jax.sharding import PartitionSpec as P

TILES_SEQ = 32
MESH = pl.DeviceIdType.MESH


def exchange_kernel(
    sizes, small_in, x_ref, gain_ref, recv_ref, keys_ref,
    small_ref, gain, small_sem, first_table, limit_table, note_out, notes, note_table, second, keys_out,
    x_sem, gain_sem, y_send, y_recv, g_send, g_recv, own_sem,
    note_send, note_recv, note_sem, key_send, key_recv, *buffers,
):
    nx, ny, depth, per_peer, chunk_rows = sizes
    chunks = len(chunk_rows)
    starts = [sum(chunk_rows[:c]) for c in range(chunks)]
    groups = nx * ny
    tiles_here, tile_rows, _ = x_ref.shape
    raw, first, arrived, outgoing = (buffers[i * chunks : (i + 1) * chunks] for i in range(4))
    gx, gy, gz = lax.axis_index("gx"), lax.axis_index("gy"), lax.axis_index("gz")
    group = gx * ny + gy
    me = group * depth + gz
    offsets = [(dx, dy) for dy in sorted(range(ny), key=lambda d: abs(d - ny // 2)) for dx in range(nx)]
    offsets.remove((0, 0))

    def load(c):
        return pltpu.make_async_copy(
            x_ref.at[:, pl.ds(starts[c], chunk_rows[c])], raw[c], x_sem.at[c]
        )

    def fill_tables():
        depths = [lax.rem(small_ref[0, i], depth) for i in range(tiles_here)]
        dest_groups = [lax.div(small_ref[0, i], depth) for i in range(tiles_here)]
        places, limits = [], []
        for i in range(tiles_here):
            spot = jnp.int32(0)
            for j in range(i):
                spot = spot + jnp.where(depths[j] == depths[i], 1, 0)
            places.append(depths[i] * per_peer + spot)
            tile = me * tiles_here + i
            length = small_ref[0, 2 * tiles_here + tile // TILES_SEQ]
            limits.append(jnp.maximum(length - tile % TILES_SEQ * tile_rows, 0))
        lane = lax.broadcasted_iota(jnp.int32, note_out.shape[1:], 1)
        for z in range(depth):
            row = jnp.zeros(note_out.shape[1:], jnp.int32)
            for p in range(per_peer):
                slot = z * per_peer + p
                tile, limit, dest_group, key = (jnp.int32(v) for v in (0, 0, -1, 0))
                for i in range(tiles_here):
                    hit = places[i] == slot
                    tile = jnp.where(hit, i, tile)
                    limit = jnp.where(hit, limits[i], limit)
                    dest_group = jnp.where(hit, dest_groups[i], dest_group)
                    key = jnp.where(hit, small_ref[0, tiles_here + i] + 1, key)
                first_table[slot] = tile
                limit_table[slot] = limit
                row = jnp.where(lane == p, dest_group, row)
                row = jnp.where(lane == per_peer + p, key, row)
            note_out[z] = row

    def normed(c, slot):
        rows = chunk_rows[c]
        values = raw[c][first_table[slot]].astype(jnp.float32)
        meansq = jnp.mean(values * values, axis=-1, keepdims=True)
        scaled = values * lax.rsqrt(jnp.maximum(meansq, 0.25)) * gain[...]
        row = starts[c] + lax.broadcasted_iota(jnp.int32, (rows, 1), 0)
        return jnp.where(row < limit_table[slot], scaled, 0.0).astype(jnp.bfloat16)

    def y_copy(c, dz, peer, origin):
        return pltpu.make_async_remote_copy(
            src_ref=first[c].at[dz - 1],
            dst_ref=arrived[c].at[pl.ds(origin * per_peer, per_peer)],
            send_sem=y_send.at[c, dz - 1],
            recv_sem=y_recv.at[c, dz - 1],
            device_id=(gx, gy, peer),
            device_id_type=MESH,
        )

    def peer_of(k):
        dx, dy = offsets[k]
        return lax.rem(gx + dx, nx), lax.rem(gy + dy, ny)

    def g_copy(c, k, px, py, origin):
        return pltpu.make_async_remote_copy(
            src_ref=outgoing[c].at[k],
            dst_ref=recv_ref.at[origin, pl.ds(starts[c], chunk_rows[c])],
            send_sem=g_send.at[c, k],
            recv_sem=g_recv.at[c, k],
            device_id=(px, py, gz),
            device_id_type=MESH,
        )

    def own_copy(c):
        return pltpu.make_async_copy(
            outgoing[c].at[groups - 1],
            recv_ref.at[group, pl.ds(starts[c], chunk_rows[c])],
            own_sem.at[c],
        )

    def note_copy(dz, peer, place):
        return pltpu.make_async_remote_copy(
            src_ref=note_out.at[peer],
            dst_ref=notes.at[place],
            send_sem=note_send.at[dz - 1],
            recv_sem=note_recv.at[dz - 1],
            device_id=(gx, gy, peer),
            device_id_type=MESH,
        )

    def key_copy(k, px, py, place):
        return pltpu.make_async_remote_copy(
            src_ref=keys_out.at[k],
            dst_ref=keys_ref.at[place],
            send_sem=key_send.at[k],
            recv_sem=key_recv.at[k],
            device_id=(px, py, gz),
            device_id_type=MESH,
        )

    def prepare(c):
        load(c).wait()
        for dz in range(1, depth):
            peer = lax.rem(gz + dz, depth)
            for p in range(per_peer):
                first[c][dz - 1, p] = normed(c, peer * per_peer + p)
        for p in range(per_peer):
            arrived[c][gz * per_peer + p] = normed(c, gz * per_peer + p)

    def send_first(c):
        for dz in range(1, depth):
            y_copy(c, dz, lax.rem(gz + dz, depth), gz).start()

    def find_slots():
        for dz in range(1, depth):
            origin = lax.rem(gz + depth - dz, depth)
            note_copy(dz, origin, origin).wait()
        tables = [
            pltpu.make_async_copy(
                notes.at[lax.rem(gz + dz, depth)], note_table.at[lax.rem(gz + dz, depth)], note_sem.at[dz]
            )
            for dz in range(1, depth)
        ]
        tables.append(pltpu.make_async_copy(note_out.at[gz], note_table.at[gz], note_sem.at[0]))
        for copy in tables:
            copy.start()
        for copy in tables:
            copy.wait()

        for k in range(groups):
            px, py = peer_of(k) if k < groups - 1 else (gx, gy)
            wanted = px * ny + py
            slot, key = jnp.int32(0), jnp.int32(0)
            for z in range(depth):
                for p in range(per_peer):
                    hit = note_table[z, 0, p] == wanted
                    slot = jnp.where(hit, z * per_peer + p, slot)
                    key = jnp.where(hit, note_table[z, 0, per_peer + p], key)
            second[k] = slot
            row = jnp.full(keys_out.shape[1:], key, jnp.int32)
            if k < groups - 1:
                keys_out[k] = row
            else:
                keys_ref[group] = row

    def forward(c):
        for dz in range(1, depth):
            origin = lax.rem(gz + depth - dz, depth)
            y_copy(c, dz, origin, origin).wait_recv()
        for k in range(groups):
            outgoing[c][k] = arrived[c][second[k]]
        for k in range(groups - 1):
            px, py = peer_of(k)
            g_copy(c, k, px, py, group).start()
        own_copy(c).start()

    small = [
        pltpu.make_async_copy(small_in, small_ref, small_sem),
        pltpu.make_async_copy(gain_ref, gain, gain_sem),
    ]
    for copy in small:
        copy.start()
    for c in range(chunks):
        load(c).start()
    barrier = pltpu.get_barrier_semaphore()
    for dz in range(1, depth):
        pl.semaphore_signal(
            barrier, inc=1, device_id=(gx, gy, lax.rem(gz + dz, depth)), device_id_type=MESH
        )
    for k in range(groups - 1):
        px, py = peer_of(k)
        pl.semaphore_signal(barrier, inc=1, device_id=(px, py, gz), device_id_type=MESH)
    for copy in small:
        copy.wait()
    fill_tables()
    prepare(0)
    pl.semaphore_wait(barrier, depth - 1 + groups - 1)
    for dz in range(1, depth):
        note_copy(dz, lax.rem(gz + dz, depth), gz).start()
    send_first(0)
    if chunks > 1:
        prepare(1)
        send_first(1)
    find_slots()
    forward(0)
    for k in range(groups - 1):
        px, py = peer_of(k)
        key_copy(k, px, py, group).start()
    for c in range(2, chunks):
        prepare(c)
        send_first(c)
        forward(c - 1)
    if chunks > 1:
        forward(chunks - 1)

    for c in range(chunks):
        for dz in range(1, depth):
            y_copy(c, dz, lax.rem(gz + dz, depth), gz).wait_send()
    sources = []
    for dx, dy in offsets:
        sources.append((lax.rem(gx + nx - dx, nx), lax.rem(gy + ny - dy, ny)))
    for k, (sx, sy) in enumerate(sources):
        key_copy(k, sx, sy, sx * ny + sy).wait()
    for c in range(chunks):
        for k, (sx, sy) in enumerate(sources):
            g_copy(c, k, sx, sy, sx * ny + sy).wait()
        own_copy(c).wait()


def place_kernel(source_ref, filled_ref, blocks_ref, out_ref, zeros, out_sem):
    cap = out_ref.shape[0]

    def store(slot):
        return pltpu.make_async_copy(blocks_ref.at[source_ref[slot]], out_ref.at[slot], out_sem.at[slot])

    for slot in range(cap):
        pl.when(filled_ref[slot] == 1)(lambda slot=slot: store(slot).start())
    zeros[...] = jnp.zeros_like(zeros)
    for slot in range(cap):

        @pl.when(filled_ref[slot] == 0)
        def _():
            pltpu.make_async_copy(zeros, out_ref.at[slot], out_sem.at[slot]).start()

    for slot in range(cap):
        store(slot).wait()


def shards(embeds, dest_device, shuffle_key, lengths, gain):
    tiles_here, tile_rows, width = embeds.shape
    nx, ny, depth = lax.axis_size("gx"), lax.axis_size("gy"), lax.axis_size("gz")
    groups = nx * ny
    per_peer = (tiles_here + depth - 1) // depth
    slots = depth * per_peer
    chunk_rows = (tile_rows,)
    if tile_rows % 128 == 0:
        chunk_rows = tuple(part * tile_rows // 16 for part in (1, 1, 2, 2, 4, 4, 2))
    chunks = len(chunk_rows)

    smem = pl.BlockSpec(memory_space=pltpu.SMEM)
    vmem = pl.BlockSpec(memory_space=pltpu.VMEM)
    hbm = pl.BlockSpec(memory_space=pl.ANY)
    lanes = -(-2 * per_peer // 128) * 128
    small = jnp.concatenate([dest_device, shuffle_key, lengths])
    small = jnp.pad(small, (0, -small.shape[0] % 128))[None, :]
    received, key_rows = pl.pallas_call(
        functools.partial(exchange_kernel, (nx, ny, depth, per_peer, chunk_rows)),
        out_shape=(
            jax.ShapeDtypeStruct((groups, tile_rows, width), jnp.bfloat16),
            jax.ShapeDtypeStruct((groups, 1, 128), jnp.int32),
        ),
        in_specs=[hbm] * 3,
        out_specs=(hbm, vmem),
        scratch_shapes=[
            pltpu.SMEM(small.shape, jnp.int32),
            pltpu.VMEM((1, width), jnp.float32),
            pltpu.SemaphoreType.DMA,
            pltpu.SMEM((slots,), jnp.int32),
            pltpu.SMEM((slots,), jnp.int32),
            pltpu.VMEM((depth, 1, lanes), jnp.int32),
            pltpu.VMEM((depth, 1, lanes), jnp.int32),
            pltpu.SMEM((depth, 1, lanes), jnp.int32),
            pltpu.SMEM((groups,), jnp.int32),
            pltpu.VMEM((groups, 1, 128), jnp.int32),
            pltpu.SemaphoreType.DMA((chunks,)),
            pltpu.SemaphoreType.DMA,
            pltpu.SemaphoreType.DMA((chunks, depth - 1)),
            pltpu.SemaphoreType.DMA((chunks, depth - 1)),
            pltpu.SemaphoreType.DMA((chunks, groups)),
            pltpu.SemaphoreType.DMA((chunks, groups)),
            pltpu.SemaphoreType.DMA((chunks,)),
            pltpu.SemaphoreType.DMA((depth,)),
            pltpu.SemaphoreType.DMA((depth,)),
            pltpu.SemaphoreType.DMA((depth,)),
            pltpu.SemaphoreType.DMA((groups,)),
            pltpu.SemaphoreType.DMA((groups,)),
        ]
        + [pltpu.VMEM((tiles_here, rows, width), jnp.bfloat16) for rows in chunk_rows]
        + [pltpu.VMEM((depth - 1, per_peer, rows, width), jnp.bfloat16) for rows in chunk_rows]
        + [pltpu.VMEM((slots, rows, width), jnp.bfloat16) for rows in chunk_rows]
        + [pltpu.VMEM((groups, rows, width), jnp.bfloat16) for rows in chunk_rows],
        compiler_params=pltpu.CompilerParams(
            collective_id=0, has_side_effects=True, vmem_limit_bytes=36 * 1024 * 1024
        ),
        name="exchange",
    )(small, embeds, gain.reshape(1, width))

    key_of = key_rows[:, 0, 0]
    valid = key_of > 0
    rank = jnp.sum((valid[None, :] & (key_of[None, :] < key_of[:, None])).astype(jnp.int32), axis=1)
    cap = 2 * tiles_here
    at = valid[None, :] & (rank[None, :] == jnp.arange(cap, dtype=jnp.int32)[:, None])
    source = jnp.sum(jnp.where(at, jnp.arange(groups, dtype=jnp.int32)[None, :], 0), axis=1).astype(jnp.int32)
    filled = jnp.sum(at.astype(jnp.int32), axis=1).astype(jnp.int32)

    return pl.pallas_call(
        place_kernel,
        out_shape=jax.ShapeDtypeStruct((cap, tile_rows, width), jnp.bfloat16),
        in_specs=[smem, smem, vmem],
        out_specs=hbm,
        scratch_shapes=[
            pltpu.VMEM((tile_rows, width), jnp.bfloat16),
            pltpu.SemaphoreType.DMA((cap,)),
        ],
        compiler_params=pltpu.CompilerParams(vmem_limit_bytes=24 * 1024 * 1024),
        name="place",
    )(source, filled, received)


def solution(mesh):
    return jax.shard_map(
        shards,
        mesh=mesh,
        in_specs=(
            P(("gx", "gy", "gz"), None, None),
            P(("gx", "gy", "gz")),
            P(("gx", "gy", "gz")),
            P(),
            P(),
        ),
        out_specs=P(("gx", "gy", "gz"), None, None),
        check_vma=False,
    )
```
